16 devices in a mesh: rep: 1, dp: 16 (over x, y, z, core).
Axes of the slice: x: 2, y: 2, z: 2, core: 2. Of those that a mesh axis runs over, the one named last changes fastest.
Arguments:
- x: bfloat16 [16, 2048, 1152], P(('rep', 'dp'))
- dy: bfloat16 [16, 2048, 1152], P(('rep', 'dp'))
- w_gate: bfloat16 [2, 1152, 4608], P(None, 'dp')
- w_up: bfloat16 [2, 1152, 4608], P(None, 'dp')
- w_down: bfloat16 [2, 4608, 1152], P(None, 'dp')
Outputs:
- output 1: bfloat16 [16, 2048, 1152], P(('rep', 'dp'))
- output 2: bfloat16 [2, 1152, 4608], P('rep', 'dp')
- output 3: bfloat16 [2, 1152, 4608], P('rep', 'dp')
- output 4: bfloat16 [2, 4608, 1152], P('rep', 'dp')
All inputs are finite; a program needn't handle non-finite values.
Results may differ from the reference program's by a relative error of at most 0.018.
Values are sent between devices in bfloat16 or wider.
A program may use at most 2 GiB of HBM per device.

```python
import jax
import jax.numpy as jnp
from jax import lax

SEQUENCES = 16
TOKENS = 2048
D = 1152
FF = 4608
LAYERS = 2
NAMES = ("w_gate", "w_up", "w_down")
SHAPES = {"w_gate": (LAYERS, D, FF), "w_up": (LAYERS, D, FF), "w_down": (LAYERS, FF, D)}


def bump(key, n, height):
    away = (jnp.arange(n, dtype=jnp.int32) - jax.random.randint(key, (), 0, n, jnp.int32)) % n
    return jnp.where(away < n // 8, height, 1.0)


def together(key, own, strength):
    shared = jax.random.normal(key, own.shape[1:], jnp.float32)
    return (own + strength * shared) * lax.rsqrt(1 + strength * strength)


def setup_inputs(seed: int = 0, part: int = 0) -> dict:
    kx, kdy, ka, kb, kz, kf, kh, kl, *kw = jax.random.split(jax.random.key(seed), 8 + len(NAMES))
    kx, kdy, ka, kb = (jax.random.fold_in(k, part) for k in (kx, kdy, ka, kb))
    shape = (SEQUENCES, TOKENS, D)
    much_x, much_dy = jax.random.uniform(kz, (2,), jnp.float32, 0.0, 1.0)
    layers = 2.0 ** jax.random.uniform(kl, (LAYERS, 1, 1), jnp.float32, -1.0, 1.0)
    x = together(ka, jax.random.normal(kx, shape, jnp.float32), much_x) * bump(kf, D, 4.0)
    dy = together(kb, jax.random.normal(kdy, shape, jnp.float32), much_dy)
    drawn = {"x": x.astype(jnp.bfloat16), "dy": (dy * (SEQUENCES * TOKENS) ** -0.5).astype(jnp.bfloat16)}
    for key, name in zip(kw, NAMES, strict=True):
        w = jax.random.normal(key, SHAPES[name], jnp.float32) * SHAPES[name][1] ** -0.5
        drawn[name] = (w * {"w_gate": 1.0, "w_up": bump(kh, FF, 4.0), "w_down": layers}[name]).astype(jnp.bfloat16)
    return drawn


def matmul(a, w):
    return jnp.dot(a, w, preferred_element_type=jnp.float32).astype(jnp.bfloat16)


def normed(h):
    wide = h.astype(jnp.float32)
    scale = lax.rsqrt(jnp.mean(wide**2, -1, keepdims=True) + 1e-6)
    return (wide * scale).astype(jnp.bfloat16)


def layer(h, w):
    a = normed(h)
    gate = jnp.dot(a, w["w_gate"], preferred_element_type=jnp.float32)
    up = jnp.dot(a, w["w_up"], preferred_element_type=jnp.float32)
    return h + matmul((jax.nn.silu(gate) * up).astype(jnp.bfloat16), w["w_down"])


def stack(weights, h):
    return lax.scan(lambda h, w: (layer(h, w), None), h, weights)[0]


def reference(x, dy, w_gate, w_up, w_down):
    weights = dict(zip(NAMES, (w_gate, w_up, w_down), strict=True))

    def take(so_far, sequence):
        h, by_y = sequence
        _, back = jax.vjp(stack, weights, h)
        by_weights, by_h = back(by_y)
        return jax.tree.map(lambda total, term: total + term.astype(jnp.float32), so_far, by_weights), by_h

    none_yet = {name: jnp.zeros(w.shape, jnp.float32) for name, w in weights.items()}
    by_weights, by_x = lax.scan(take, none_yet, (x, dy))
    return (by_x, *(by_weights[name].astype(jnp.bfloat16) for name in NAMES))
```

```python
import jax
import jax.numpy as jnp
from jax import lax
from jax.sharding import PartitionSpec as P

F32 = jnp.float32
BF16 = jnp.bfloat16


def mm(a, b, ca, cb):
    return lax.dot_general(a, b, (((ca,), (cb,)), ((), ())), preferred_element_type=F32)


def normed(h):
    wide = h.astype(F32)
    scale = lax.rsqrt(jnp.mean(wide**2, -1, keepdims=True) + 1e-6)
    return (wide * scale).astype(BF16), scale


def norm_back(h, scale, da, dh):
    wide = h.astype(F32)
    da = da.astype(F32)
    inner = jnp.mean(da * wide, -1, keepdims=True)
    return (dh.astype(F32) + scale * (da - wide * (scale * scale * inner))).astype(BF16)


def gather(w):
    return lax.all_gather(w, "dp", axis=0, tiled=True)


def scatter(dw):
    return lax.psum_scatter(dw, "dp", scatter_dimension=0, tiled=True)


def local(x, dy, w_gate, w_up, w_down):
    layers = w_gate.shape[0]
    h, dh = x[0], dy[0]
    wg = [gather(w_gate[n]) for n in range(layers)]
    wu = [gather(w_up[n]) for n in range(layers)]
    wd = [gather(w_down[n]) for n in range(layers)]
    saved = []
    for n in range(layers):
        a, scale = normed(h)
        gate = mm(a, wg[n], 1, 0)
        up = mm(a, wu[n], 1, 0)
        act = (jax.nn.silu(gate) * up).astype(BF16)
        saved.append((h, scale, a, gate, up, act))
        if n < layers - 1:
            h = h + mm(act, wd[n], 1, 0).astype(BF16)
    grads = [[None] * layers for _ in range(3)]
    for n in reversed(range(layers)):
        h, scale, a, gate, up, act = saved[n]
        grads[2][n] = scatter(mm(act, dh, 0, 0).astype(BF16))
        dact = mm(dh, wd[n], 1, 1).astype(BF16).astype(F32)
        s = jax.nn.sigmoid(gate)
        dup = (dact * (gate * s)).astype(BF16)
        dgate = (dact * up * (s * (1 + gate * (1 - s)))).astype(BF16)
        grads[0][n] = scatter(mm(a, dgate, 0, 0).astype(BF16))
        grads[1][n] = scatter(mm(a, dup, 0, 0).astype(BF16))
        da = mm(dgate, wg[n], 1, 1).astype(BF16).astype(F32) + mm(dup, wu[n], 1, 1).astype(BF16).astype(F32)
        dh = norm_back(h, scale, da, dh)
    return (dh[None], *(jnp.stack(g) for g in grads))


def solution(mesh):
    seq = P(("rep", "dp"), None, None)
    w = P(None, "dp", None)
    out = P("rep", "dp", None)
    return jax.shard_map(local, mesh=mesh, in_specs=(seq, seq, w, w, w), out_specs=(seq, out, out, out), check_vma=False)
```

```python
import jax
import jax.numpy as jnp
from jax import lax
from jax.experimental import pallas as pl
from jax.experimental.pallas import tpu as pltpu
from jax.sharding import Mesh, PartitionSpec as P

F32 = jnp.float32
BF16 = jnp.bfloat16
SWAP = ((0, 1), (1, 0))
EPS = 1e-6


chain = []


def after(t, *first):
    return lax.optimization_barrier((t, *first))[0]


def dot(a, b, ca, cb):
    return lax.dot_general(a, b, (((ca,), (cb,)), ((), ())), preferred_element_type=F32)


def call(kernel, grid, ins, outs, flops, args, scratch=(), prefetch=None):
    def spec(given):
        if given is None:
            return pl.BlockSpec(memory_space=pl.ANY)
        block, index, buffers = given
        return pl.BlockSpec(block, index, pipeline_mode=pl.Buffered(buffers)) if buffers else pl.BlockSpec(block, index)

    args = (after(args[0], *chain), *args[1:])
    size = sum(a.size * a.dtype.itemsize for a in args) + sum(s[0] * s[1] * jnp.dtype(d).itemsize for s, d, _, _ in outs)
    results = pl.pallas_call(
        kernel,
        grid_spec=pltpu.PrefetchScalarGridSpec(
            num_scalar_prefetch=0 if prefetch is None else 1,
            grid=grid,
            in_specs=[spec(given) for given in ins],
            out_specs=[pl.BlockSpec(block, index) for _, _, block, index in outs],
            scratch_shapes=list(scratch),
        ),
        out_shape=[jax.ShapeDtypeStruct(shape, dtype) for shape, dtype, _, _ in outs],
        cost_estimate=pl.CostEstimate(flops=flops, bytes_accessed=size, transcendentals=0),
        compiler_params=pltpu.CompilerParams(dimension_semantics=("arbitrary",) * len(grid), vmem_limit_bytes=60 << 20),
    )(*([] if prefetch is None else [prefetch]), *args)
    chain[:] = results[:1]
    return results


def norm_of(wide):
    scale = lax.rsqrt(jnp.mean(wide * wide, -1, keepdims=True) + EPS)
    return (wide * scale).astype(BF16), scale


def norm_kernel(h, a, a_turned):
    value = norm_of(h[...].astype(F32))[0]
    a[...] = value
    a_turned[...] = value.astype(F32).T.astype(BF16)


def normed(h):
    rows, d = h.shape
    m = rows // 4
    at, across = lambda i: (i, 0), lambda i: (0, i)
    return call(
        norm_kernel,
        (4,),
        [((m, d), at, 0)],
        [((rows, d), BF16, (m, d), at), ((d, rows), BF16, (d, m), across)],
        4 * rows * d,
        (h,),
    )


def sigmoid(x):
    return 0.5 + 0.5 * jnp.tanh(0.5 * x)


def gate_kernel(a, w, gate):
    gate[...] = dot(a[...], w[...], 1, 0)


def up_kernel(a, w, gate, up, act):
    value = dot(a[...], w[...], 1, 0)
    g = gate[...]
    up[...] = value
    act[...] = (g * sigmoid(g) * value).astype(BF16)


def back_of(g, up, dact):
    s = sigmoid(g)
    silu = g * s
    return (dact * up * (s + silu * (1 - s))).astype(BF16), (dact * silu).astype(BF16), silu


def up_back_kernel(a, w, gate, dact, act, dgate, dup):
    value = dot(a[...], w[...], 1, 0)
    dg, du, silu = back_of(gate[...], value, dact[...].astype(F32))
    act[...] = (silu * value).astype(BF16)
    dgate[...] = dg
    dup[...] = du


def dact_kernel(dh, w, dact):
    dact[...] = dot(dh[...], w[...], 1, 1).astype(BF16)


def back_kernel(dh, w, gate, up, dgate, dup):
    dact = dot(dh[...], w[...], 1, 1).astype(BF16).astype(F32)
    dgate[...], dup[...], _ = back_of(gate[...], up[...], dact)


def wide_call(kernel, a, w, down, extras, dtypes):
    rows, d = a.shape
    hidden = w.shape[0 if down else 1]
    n = 512
    at = lambda j: (0, j)
    w_in = ((n, d), lambda j: (j, 0), 0) if down else ((d, n), at, 0)
    return call(
        kernel,
        (hidden // n,),
        [((rows, d), lambda j: (0, 0), 1), w_in] + [((rows, n), at, 0)] * len(extras),
        [((rows, hidden), dtype, (rows, n), at) for dtype in dtypes],
        2 * rows * d * hidden,
        (a, w, *extras),
    )


def down_kernel(h, act, w, out, a, a_turned):
    h_out = h[...] + dot(act[...], w[...], 1, 0).astype(BF16)
    out[...] = h_out
    norm_kernel(out, a, a_turned)


def down(h, act, w):
    rows, d = h.shape
    hidden = w.shape[0]
    m = rows // 4
    at, across = lambda i: (i, 0), lambda i: (0, i)
    return call(
        down_kernel,
        (4,),
        [((m, d), at, 0), ((m, hidden), at, 0), ((hidden, d), lambda i: (0, 0), 1)],
        [((rows, d), BF16, (m, d), at)] * 2 + [((d, rows), BF16, (d, m), across)],
        2 * rows * d * hidden,
        (h, act, w),
    )


def da_kernel(dgate, wg, dup, wu, h_hbm, dh_hbm, out, total, h, dh, sems):
    step, last = pl.program_id(0), pl.num_programs(0) - 1
    copies = [pltpu.make_async_copy(h_hbm, h, sems.at[0]), pltpu.make_async_copy(dh_hbm, dh, sems.at[1])]

    @pl.when(step == 0)
    def _():
        for copy in copies:
            copy.start()
        total[...] = jnp.zeros_like(total)

    total[...] += dot(dgate[...], wg[...], 1, 1) + dot(dup[...], wu[...], 1, 1)

    @pl.when(step == last)
    def _():
        for copy in copies:
            copy.wait()
        da = total[...].astype(BF16).astype(F32)
        wide = h[...].astype(F32)
        scale = norm_of(wide)[1]
        inner = jnp.mean(da * wide, -1, keepdims=True)
        out[...] = (dh[...].astype(F32) + scale * (da - wide * (scale * scale * inner))).astype(BF16)


def da_of(h, dh, dgate, dup, wg, wu):
    rows, d = h.shape
    hidden = wg.shape[1]
    n = 512
    at = lambda j: (0, j)
    return call(
        da_kernel,
        (hidden // n,),
        [((rows, n), at, 0), ((d, n), at, 0)] * 2 + [None] * 2,
        [((rows, d), BF16, (rows, d), lambda j: (0, 0))],
        4 * rows * d * hidden,
        (dgate, wg, dup, wu, h, dh),
        scratch=[
            pltpu.VMEM((rows, d), F32),
            pltpu.VMEM((rows, d), BF16),
            pltpu.VMEM((rows, d), BF16),
            pltpu.SemaphoreType.DMA((2,)),
        ],
    )[0]


def dw_wide_kernel(half, a_turned, b, *more):
    value = dot(a_turned[...], b[...], 1, 0)
    if len(more) == 2:
        value += more[0][...].astype(F32)
    more[-1][...] = value.astype(BF16)


def dw_tall_kernel(half, a, b, *more):
    value = dot(a[...], b[...], 0, 0)
    if len(more) == 2:
        value += more[0][...].astype(F32)
    more[-1][...] = value.astype(BF16)


def dw_wide(a_turned, b, half, theirs=None):
    d, rows = a_turned.shape
    n = 768
    count = b.shape[1] // 2
    more = [] if theirs is None else [theirs]
    at = lambda i, half: (0, i)
    return call(
        dw_wide_kernel,
        (count // n,),
        [((d, rows), lambda i, half: (0, 0), 1), ((rows, n), lambda i, half: (0, half[0] * (count // n) + i), 0)]
        + [((d, n), at, 0)] * len(more),
        [((d, count), BF16, (d, n), at)],
        2 * rows * d * count,
        (a_turned, b, *more),
        prefetch=half,
    )[0]


def dw_tall(a, b, half, theirs=None):
    rows, d = b.shape
    m = 768
    count = a.shape[1] // 2
    more = [] if theirs is None else [theirs]
    at = lambda i, half: (i, 0)
    return call(
        dw_tall_kernel,
        (count // m,),
        [((rows, m), lambda i, half: (0, half[0] * (count // m) + i), 0), ((rows, d), lambda i, half: (0, 0), 1)]
        + [((m, d), at, 0)] * len(more),
        [((count, d), BF16, (m, d), at)],
        2 * rows * d * count,
        (a, b, *more),
        prefetch=half,
    )[0]


def swap(t):
    return lax.ppermute(t, "core", SWAP)


def gather(w):
    return lax.all_gather(w, ("chip", "core"), axis=0, tiled=True)


def scatter(dw):
    return lax.psum_scatter(dw, "chip", scatter_dimension=0, tiled=True)


def local(x, dy, w_gate, w_up, w_down):
    core = lax.axis_index("core")
    chips = lax.axis_size("chip")
    mine, other = core.astype(jnp.int32)[None], (1 - core).astype(jnp.int32)[None]

    def own_wide(dw):
        rows = dw.shape[0] // 2
        top, bottom = dw[:rows], dw[rows:]
        theirs = swap(jnp.where(core == 0, bottom, top))
        own = jnp.where(core == 0, top, bottom)
        return jnp.concatenate((jnp.where(core == 0, own, theirs), jnp.where(core == 0, theirs, own)), 1)

    def own_tall(dw):
        return lax.ppermute(dw, ("chip", "core"), [(2 * k + c, chips * c + k) for k in range(chips) for c in range(2)])

    chain.clear()
    x, dy = x[0], dy[0]
    d1 = gather(w_down[1])
    a0, a0_turned = normed(x)
    g0 = gather(after(w_gate[0], a0))
    (dact1,) = wide_call(dact_kernel, dy, d1, True, (), (BF16,))
    u0 = gather(after(w_up[0], d1))
    (gate0,) = wide_call(gate_kernel, a0, g0, False, (), (F32,))
    d0 = gather(after(w_down[0], dact1))
    up0, act0 = wide_call(up_kernel, a0, u0, False, (gate0,), (F32, BF16))
    g1 = gather(after(w_gate[1], gate0))
    h1, a1, a1_turned = down(x, act0, d0)
    u1 = gather(after(w_up[1], up0))
    (gate1,) = wide_call(gate_kernel, a1, g1, False, (), (F32,))
    act1, dgate1, dup1 = wide_call(up_back_kernel, a1, u1, False, (gate1, dact1), (BF16,) * 3)

    def terms(act, a_turned, dh, dgate, dup):
        down_theirs = dw_tall(act, dh, other)
        gate_theirs = dw_wide(a_turned, dgate, other)
        down_mine = dw_tall(act, dh, mine, swap(down_theirs))
        up_theirs = dw_wide(a_turned, dup, other)
        gate_mine = dw_wide(a_turned, dgate, mine, swap(gate_theirs))
        up_mine = dw_wide(a_turned, dup, mine, swap(up_theirs))
        return [scatter(t) for t in (down_mine, gate_mine, up_mine)]

    rs_d1, rs_g1, rs_u1 = terms(act1, a1_turned, dy, dgate1, dup1)
    dh1 = da_of(h1, dy, dgate1, dup1, g1, u1)
    dgate0, dup0 = wide_call(back_kernel, dh1, d0, True, (gate0, up0), (BF16,) * 2)
    rs_d0, rs_g0, rs_u0 = terms(act0, a0_turned, dh1, dgate0, dup0)
    dx = da_of(x, dh1, dgate0, dup0, g0, u0)
    return (
        dx[None],
        jnp.stack((own_wide(rs_g0), own_wide(rs_g1))),
        jnp.stack((own_wide(rs_u0), own_wide(rs_u1))),
        jnp.stack((own_tall(rs_d0), own_tall(rs_d1))),
    )


def solution(mesh):
    cores = Mesh(mesh.devices.reshape(mesh.shape["rep"], -1, 2), ("rep", "chip", "core"))
    dp = ("chip", "core")
    seq = P(("rep", *dp), None, None)
    w = P(None, dp, None)
    out = P("rep", dp, None)
    return jax.shard_map(local, mesh=cores, in_specs=(seq, seq, w, w, w), out_specs=(seq, out, out, out), check_vma=False)
```

```python
import jax
import jax.numpy as jnp
from jax import lax
from jax.experimental import pallas as pl
from jax.experimental.pallas import tpu as pltpu
from jax.sharding import Mesh, PartitionSpec as P

F32 = jnp.float32
BF16 = jnp.bfloat16
SWAP = ((0, 1), (1, 0))
EPS = 1e-6


chain = []


def after(t, *first):
    return lax.optimization_barrier((t, *first))[0]


def dot(a, b, ca, cb):
    return lax.dot_general(a, b, (((ca,), (cb,)), ((), ())), preferred_element_type=F32)


def call(kernel, grid, ins, outs, flops, args, scratch=(), prefetch=None):
    def spec(given):
        if given is None:
            return pl.BlockSpec(memory_space=pl.ANY)
        block, index, buffers = given
        return pl.BlockSpec(block, index, pipeline_mode=pl.Buffered(buffers)) if buffers else pl.BlockSpec(block, index)

    args = (after(args[0], *chain), *args[1:])
    size = sum(a.size * a.dtype.itemsize for a in args) + sum(s[0] * s[1] * jnp.dtype(d).itemsize for s, d, _, _ in outs)
    results = pl.pallas_call(
        kernel,
        grid_spec=pltpu.PrefetchScalarGridSpec(
            num_scalar_prefetch=0 if prefetch is None else 1,
            grid=grid,
            in_specs=[spec(given) for given in ins],
            out_specs=[pl.BlockSpec(block, index) for _, _, block, index in outs],
            scratch_shapes=list(scratch),
        ),
        out_shape=[jax.ShapeDtypeStruct(shape, dtype) for shape, dtype, _, _ in outs],
        cost_estimate=pl.CostEstimate(flops=flops, bytes_accessed=size, transcendentals=0),
        compiler_params=pltpu.CompilerParams(dimension_semantics=("arbitrary",) * len(grid), vmem_limit_bytes=60 << 20),
    )(*([] if prefetch is None else [prefetch]), *args)
    chain[:] = results[:1]
    return results


def norm_of(wide):
    scale = lax.rsqrt(jnp.mean(wide * wide, -1, keepdims=True) + EPS)
    return (wide * scale).astype(BF16), scale


def norm_kernel(h, a, a_turned):
    value = norm_of(h[...].astype(F32))[0]
    a[...] = value
    a_turned[...] = value.astype(F32).T.astype(BF16)


def normed(h):
    rows, d = h.shape
    m = rows // 4
    at, across = lambda i: (i, 0), lambda i: (0, i)
    return call(
        norm_kernel,
        (4,),
        [((m, d), at, 0)],
        [((rows, d), BF16, (m, d), at), ((d, rows), BF16, (d, m), across)],
        4 * rows * d,
        (h,),
    )


def sigmoid(x):
    return 0.5 + 0.5 * jnp.tanh(0.5 * x)


def gate_kernel(a, w, gate):
    gate[...] = dot(a[...], w[...], 1, 0)


def up_kernel(a, w, gate, up, act):
    value = dot(a[...], w[...], 1, 0)
    g = gate[...]
    up[...] = value
    act[...] = (g * sigmoid(g) * value).astype(BF16)


def back_of(g, up, dact):
    s = sigmoid(g)
    silu = g * s
    return (dact * up * (s + silu * (1 - s))).astype(BF16), (dact * silu).astype(BF16), silu


def back_kernel(dh, w, gate, up, dgate, dup):
    dact = dot(dh[...], w[...], 1, 1).astype(BF16).astype(F32)
    dgate[...], dup[...], _ = back_of(gate[...], up[...], dact)


def wide_call(kernel, a, w, down, extras, dtypes):
    rows, d = a.shape
    hidden = w.shape[0 if down else 1]
    n = 512
    at = lambda j: (0, j)
    w_in = ((n, d), lambda j: (j, 0), 0) if down else ((d, n), at, 0)
    return call(
        kernel,
        (hidden // n,),
        [((rows, d), lambda j: (0, 0), 1), w_in] + [((rows, n), at, 0)] * len(extras),
        [((rows, hidden), dtype, (rows, n), at) for dtype in dtypes],
        2 * rows * d * hidden,
        (a, w, *extras),
    )


def down_kernel(h, act, w, out, a, a_turned):
    h_out = h[...] + dot(act[...], w[...], 1, 0).astype(BF16)
    out[...] = h_out
    norm_kernel(out, a, a_turned)


def down(h, act, w):
    rows, d = h.shape
    hidden = w.shape[0]
    m = rows // 4
    at, across = lambda i: (i, 0), lambda i: (0, i)
    return call(
        down_kernel,
        (4,),
        [((m, d), at, 0), ((m, hidden), at, 0), ((hidden, d), lambda i: (0, 0), 1)],
        [((rows, d), BF16, (m, d), at)] * 2 + [((d, rows), BF16, (d, m), across)],
        2 * rows * d * hidden,
        (h, act, w),
    )


def da_kernel(dgate, wg, dup, wu, h_hbm, dh_hbm, out, total, h, dh, sems):
    step, last = pl.program_id(0), pl.num_programs(0) - 1
    copies = [pltpu.make_async_copy(h_hbm, h, sems.at[0]), pltpu.make_async_copy(dh_hbm, dh, sems.at[1])]

    @pl.when(step == 0)
    def _():
        for copy in copies:
            copy.start()
        total[...] = jnp.zeros_like(total)

    total[...] += dot(dgate[...], wg[...], 1, 1) + dot(dup[...], wu[...], 1, 1)

    @pl.when(step == last)
    def _():
        for copy in copies:
            copy.wait()
        da = total[...].astype(BF16).astype(F32)
        wide = h[...].astype(F32)
        scale = norm_of(wide)[1]
        inner = jnp.mean(da * wide, -1, keepdims=True)
        out[...] = (dh[...].astype(F32) + scale * (da - wide * (scale * scale * inner))).astype(BF16)


def da_of(h, dh, dgate, dup, wg, wu):
    rows, d = h.shape
    hidden = wg.shape[1]
    n = 512
    at = lambda j: (0, j)
    return call(
        da_kernel,
        (hidden // n,),
        [((rows, n), at, 0), ((d, n), at, 0)] * 2 + [None] * 2,
        [((rows, d), BF16, (rows, d), lambda j: (0, 0))],
        4 * rows * d * hidden,
        (dgate, wg, dup, wu, h, dh),
        scratch=[
            pltpu.VMEM((rows, d), F32),
            pltpu.VMEM((rows, d), BF16),
            pltpu.VMEM((rows, d), BF16),
            pltpu.SemaphoreType.DMA((2,)),
        ],
    )[0]


def dw_wide_kernel(half, a_turned, b, *more):
    value = dot(a_turned[...], b[...], 1, 0)
    if len(more) == 2:
        value += more[0][...].astype(F32)
    more[-1][...] = value.astype(BF16)


def dw_tall_kernel(half, a, b, *more):
    value = dot(a[...], b[...], 0, 0)
    if len(more) == 2:
        value += more[0][...].astype(F32)
    more[-1][...] = value.astype(BF16)


def dw_wide(a_turned, b, half, theirs=None):
    d, rows = a_turned.shape
    n = 768
    count = b.shape[1] // 2
    more = [] if theirs is None else [theirs]
    at = lambda i, half: (0, i)
    return call(
        dw_wide_kernel,
        (count // n,),
        [((d, rows), lambda i, half: (0, 0), 1), ((rows, n), lambda i, half: (0, half[0] * (count // n) + i), 0)]
        + [((d, n), at, 0)] * len(more),
        [((d, count), BF16, (d, n), at)],
        2 * rows * d * count,
        (a_turned, b, *more),
        prefetch=half,
    )[0]


def dw_tall(a, b, half, theirs=None):
    rows, d = b.shape
    m = 768
    count = a.shape[1] // 2
    more = [] if theirs is None else [theirs]
    at = lambda i, half: (i, 0)
    return call(
        dw_tall_kernel,
        (count // m,),
        [((rows, m), lambda i, half: (0, half[0] * (count // m) + i), 0), ((rows, d), lambda i, half: (0, 0), 1)]
        + [((m, d), at, 0)] * len(more),
        [((count, d), BF16, (m, d), at)],
        2 * rows * d * count,
        (a, b, *more),
        prefetch=half,
    )[0]


def interleave_kernel(core, blocks, theirs, out):
    rows = blocks.shape[1]
    own, far = blocks[0], theirs[0]
    first = core[0] == 0
    out[:rows, :] = jnp.where(first, own, far)
    out[rows:, :] = jnp.where(first, far, own)


def interleave(blocks, theirs, core):
    chips, rows, d = blocks.shape
    block = (1, rows, d), lambda k, core: (k, 0, 0), 0
    return call(
        interleave_kernel,
        (chips,),
        [block, block],
        [((2 * chips * rows, d), BF16, (2 * rows, d), lambda k, core: (k, 0))],
        chips * rows * d,
        (blocks, theirs),
        prefetch=core,
    )[0]


def swap(t):
    return lax.ppermute(t, "core", SWAP)


def gather(w):
    return lax.all_gather(w, ("chip", "core"), axis=0, tiled=True)


def scatter(dw):
    return lax.psum_scatter(dw, "chip", scatter_dimension=0, tiled=True)


def local(x, dy, w_gate, w_up, w_down):
    core = lax.axis_index("core")
    chips = lax.axis_size("chip")
    mine, other = core.astype(jnp.int32)[None], (1 - core).astype(jnp.int32)[None]

    def own_wide(dw):
        rows = dw.shape[0] // 2
        top, bottom = dw[:rows], dw[rows:]
        theirs = swap(jnp.where(core == 0, bottom, top))
        own = jnp.where(core == 0, top, bottom)
        return jnp.concatenate((jnp.where(core == 0, own, theirs), jnp.where(core == 0, theirs, own)), 1)

    def own_tall(dw):
        return lax.ppermute(dw, ("chip", "core"), [(2 * k + c, chips * c + k) for k in range(chips) for c in range(2)])

    def gather_beside(w):
        chip = lax.axis_index("chip")
        blocks, bit = w[None], 1
        while bit < chips:
            theirs = lax.ppermute(blocks, "chip", [(k, k ^ bit) for k in range(chips)])
            low = (chip & bit) == 0
            blocks = jnp.concatenate((jnp.where(low, blocks, theirs), jnp.where(low, theirs, blocks)))
            bit *= 2
        theirs = swap(blocks)
        return blocks, theirs

    chain.clear()
    x, dy = x[0], dy[0]
    g0 = gather(w_gate[0])
    d0 = gather_beside(w_down[0])
    a0, a0_turned = normed(x)
    u0 = gather(after(w_up[0], a0))
    (gate0,) = wide_call(gate_kernel, a0, g0, False, (), (F32,))
    g1 = gather(after(w_gate[1], gate0))
    up0, act0 = wide_call(up_kernel, a0, u0, False, (gate0,), (F32, BF16))
    u1 = gather(after(w_up[1], up0))
    d0 = interleave(*d0, mine)
    h1, a1, a1_turned = down(x, act0, d0)
    d1 = gather(after(w_down[1], h1))
    (gate1,) = wide_call(gate_kernel, a1, g1, False, (), (F32,))
    up1, act1 = wide_call(up_kernel, a1, u1, False, (gate1,), (F32, BF16))

    def back(act, a_turned, dh, w, gate, up):
        down_theirs = dw_tall(act, dh, other)
        dgate, dup = wide_call(back_kernel, dh, w, True, (gate, up), (BF16,) * 2)
        down_mine = dw_tall(act, dh, mine, swap(down_theirs))
        gate_theirs = dw_wide(a_turned, dgate, other)
        up_theirs = dw_wide(a_turned, dup, other)
        gate_mine = dw_wide(a_turned, dgate, mine, swap(gate_theirs))
        up_mine = dw_wide(a_turned, dup, mine, swap(up_theirs))
        return dgate, dup, *(scatter(t) for t in (down_mine, gate_mine, up_mine))

    dgate1, dup1, rs_d1, rs_g1, rs_u1 = back(act1, a1_turned, dy, d1, gate1, up1)
    dh1 = da_of(h1, dy, dgate1, dup1, g1, u1)
    dgate0, dup0, rs_d0, rs_g0, rs_u0 = back(act0, a0_turned, dh1, d0, gate0, up0)
    dx = da_of(x, dh1, dgate0, dup0, g0, u0)
    return (
        dx[None],
        jnp.stack((own_wide(rs_g0), own_wide(rs_g1))),
        jnp.stack((own_wide(rs_u0), own_wide(rs_u1))),
        jnp.stack((own_tall(rs_d0), own_tall(rs_d1))),
    )


def solution(mesh):
    cores = Mesh(mesh.devices.reshape(mesh.shape["rep"], -1, 2), ("rep", "chip", "core"))
    dp = ("chip", "core")
    seq = P(("rep", *dp), None, None)
    w = P(None, dp, None)
    out = P("rep", dp, None)
    return jax.shard_map(local, mesh=cores, in_specs=(seq, seq, w, w, w), out_specs=(seq, out, out, out), check_vma=False)
```

```python
import jax
import jax.numpy as jnp
from jax import lax
from jax.experimental import pallas as pl
from jax.experimental.pallas import tpu as pltpu
from jax.sharding import Mesh, PartitionSpec as P

F32 = jnp.float32
BF16 = jnp.bfloat16
SWAP = ((0, 1), (1, 0))
EPS = 1e-6


chain = []


def after(t, *first):
    return lax.optimization_barrier((t, *first))[0]


def dot(a, b, ca, cb):
    return lax.dot_general(a, b, (((ca,), (cb,)), ((), ())), preferred_element_type=F32)


def call(kernel, grid, ins, outs, flops, args, scratch=(), prefetch=None):
    def spec(given):
        if given is None:
            return pl.BlockSpec(memory_space=pl.ANY)
        block, index, buffers = given
        return pl.BlockSpec(block, index, pipeline_mode=pl.Buffered(buffers)) if buffers else pl.BlockSpec(block, index)

    args = (after(args[0], *chain), *args[1:])
    size = sum(a.size * a.dtype.itemsize for a in args) + sum(s[0] * s[1] * jnp.dtype(d).itemsize for s, d, _, _ in outs)
    results = pl.pallas_call(
        kernel,
        grid_spec=pltpu.PrefetchScalarGridSpec(
            num_scalar_prefetch=0 if prefetch is None else 1,
            grid=grid,
            in_specs=[spec(given) for given in ins],
            out_specs=[pl.BlockSpec(block, index) for _, _, block, index in outs],
            scratch_shapes=list(scratch),
        ),
        out_shape=[jax.ShapeDtypeStruct(shape, dtype) for shape, dtype, _, _ in outs],
        cost_estimate=pl.CostEstimate(flops=flops, bytes_accessed=size, transcendentals=0),
        compiler_params=pltpu.CompilerParams(dimension_semantics=("arbitrary",) * len(grid), vmem_limit_bytes=60 << 20),
    )(*([] if prefetch is None else [prefetch]), *args)
    chain[:] = results[:1]
    return results


def norm_of(wide):
    scale = lax.rsqrt(jnp.mean(wide * wide, -1, keepdims=True) + EPS)
    return (wide * scale).astype(BF16), scale


def norm_kernel(h, a, a_turned):
    value = norm_of(h[...].astype(F32))[0]
    a[...] = value
    a_turned[...] = value.astype(F32).T.astype(BF16)


def normed(h):
    rows, d = h.shape
    m = rows // 4
    at, across = lambda i: (i, 0), lambda i: (0, i)
    return call(
        norm_kernel,
        (4,),
        [((m, d), at, 0)],
        [((rows, d), BF16, (m, d), at), ((d, rows), BF16, (d, m), across)],
        4 * rows * d,
        (h,),
    )


def sigmoid(x):
    return 0.5 + 0.5 * jnp.tanh(0.5 * x)


def gate_kernel(a, w, gate):
    gate[...] = dot(a[...], w[...], 1, 0)


def up_kernel(a, w, gate, up, act):
    value = dot(a[...], w[...], 1, 0)
    g = gate[...]
    up[...] = value
    act[...] = (g * sigmoid(g) * value).astype(BF16)


def back_of(g, up, dact):
    s = sigmoid(g)
    silu = g * s
    return (dact * up * (s + silu * (1 - s))).astype(BF16), (dact * silu).astype(BF16), silu


def back_kernel(dh, w, gate, up, dgate, dup):
    dact = dot(dh[...], w[...], 1, 1).astype(BF16).astype(F32)
    dgate[...], dup[...], _ = back_of(gate[...], up[...], dact)


def wide_call(kernel, a, w, down, extras, dtypes):
    rows, d = a.shape
    hidden = w.shape[0 if down else 1]
    n = 512
    at = lambda j: (0, j)
    w_in = ((n, d), lambda j: (j, 0), 0) if down else ((d, n), at, 0)
    return call(
        kernel,
        (hidden // n,),
        [((rows, d), lambda j: (0, 0), 1), w_in] + [((rows, n), at, 0)] * len(extras),
        [((rows, hidden), dtype, (rows, n), at) for dtype in dtypes],
        2 * rows * d * hidden,
        (a, w, *extras),
    )


def down_kernel(h, act, w, out, a, a_turned):
    h_out = h[...] + dot(act[...], w[...], 1, 0).astype(BF16)
    out[...] = h_out
    norm_kernel(out, a, a_turned)


def down(h, act, w):
    rows, d = h.shape
    hidden = w.shape[0]
    m = rows // 4
    at, across = lambda i: (i, 0), lambda i: (0, i)
    return call(
        down_kernel,
        (4,),
        [((m, d), at, 0), ((m, hidden), at, 0), ((hidden, d), lambda i: (0, 0), 1)],
        [((rows, d), BF16, (m, d), at)] * 2 + [((d, rows), BF16, (d, m), across)],
        2 * rows * d * hidden,
        (h, act, w),
    )


def da_kernel(dgate, wg, dup, wu, h_hbm, dh_hbm, out, total, h, dh, sems):
    step, last = pl.program_id(0), pl.num_programs(0) - 1
    copies = [pltpu.make_async_copy(h_hbm, h, sems.at[0]), pltpu.make_async_copy(dh_hbm, dh, sems.at[1])]

    @pl.when(step == 0)
    def _():
        for copy in copies:
            copy.start()
        total[...] = jnp.zeros_like(total)

    total[...] += dot(dgate[...], wg[...], 1, 1) + dot(dup[...], wu[...], 1, 1)

    @pl.when(step == last)
    def _():
        for copy in copies:
            copy.wait()
        da = total[...].astype(BF16).astype(F32)
        wide = h[...].astype(F32)
        scale = norm_of(wide)[1]
        inner = jnp.mean(da * wide, -1, keepdims=True)
        out[...] = (dh[...].astype(F32) + scale * (da - wide * (scale * scale * inner))).astype(BF16)


def da_of(h, dh, dgate, dup, wg, wu):
    rows, d = h.shape
    hidden = wg.shape[1]
    n = 512
    at = lambda j: (0, j)
    return call(
        da_kernel,
        (hidden // n,),
        [((rows, n), at, 0), ((d, n), at, 0)] * 2 + [None] * 2,
        [((rows, d), BF16, (rows, d), lambda j: (0, 0))],
        4 * rows * d * hidden,
        (dgate, wg, dup, wu, h, dh),
        scratch=[
            pltpu.VMEM((rows, d), F32),
            pltpu.VMEM((rows, d), BF16),
            pltpu.VMEM((rows, d), BF16),
            pltpu.SemaphoreType.DMA((2,)),
        ],
    )[0]


def dw_wide_kernel(half, a_turned, b, *more):
    value = dot(a_turned[...], b[...], 1, 0)
    if len(more) == 2:
        value += more[0][...].astype(F32)
    more[-1][...] = value.astype(BF16)


def dw_tall_kernel(half, a, b, *more):
    value = dot(a[...], b[...], 0, 0)
    if len(more) == 2:
        value += more[0][...].astype(F32)
    more[-1][...] = value.astype(BF16)


def dw_wide(a_turned, b, half, theirs=None):
    d, rows = a_turned.shape
    n = 768
    count = b.shape[1] // 2
    more = [] if theirs is None else [theirs]
    at = lambda i, half: (0, i)
    return call(
        dw_wide_kernel,
        (count // n,),
        [((d, rows), lambda i, half: (0, 0), 1), ((rows, n), lambda i, half: (0, half[0] * (count // n) + i), 0)]
        + [((d, n), at, 0)] * len(more),
        [((d, count), BF16, (d, n), at)],
        2 * rows * d * count,
        (a_turned, b, *more),
        prefetch=half,
    )[0]


def dw_tall(a, b, half, theirs=None):
    rows, d = b.shape
    m = 768
    count = a.shape[1] // 2
    more = [] if theirs is None else [theirs]
    at = lambda i, half: (i, 0)
    return call(
        dw_tall_kernel,
        (count // m,),
        [((rows, m), lambda i, half: (0, half[0] * (count // m) + i), 0), ((rows, d), lambda i, half: (0, 0), 1)]
        + [((m, d), at, 0)] * len(more),
        [((count, d), BF16, (m, d), at)],
        2 * rows * d * count,
        (a, b, *more),
        prefetch=half,
    )[0]


def swap(t):
    return lax.ppermute(t, "core", SWAP)


def gather(w):
    return lax.all_gather(w, ("chip", "core"), axis=0, tiled=True)


def scatter(dw):
    return lax.psum_scatter(dw, "chip", scatter_dimension=0, tiled=True)


def local(x, dy, w_gate, w_up, w_down):
    core = lax.axis_index("core")
    chips = lax.axis_size("chip")
    mine, other = core.astype(jnp.int32)[None], (1 - core).astype(jnp.int32)[None]

    def own_wide(dw):
        rows = dw.shape[0] // 2
        top, bottom = dw[:rows], dw[rows:]
        theirs = swap(jnp.where(core == 0, bottom, top))
        own = jnp.where(core == 0, top, bottom)
        return jnp.concatenate((jnp.where(core == 0, own, theirs), jnp.where(core == 0, theirs, own)), 1)

    def own_tall(dw):
        return lax.ppermute(dw, ("chip", "core"), [(2 * k + c, chips * c + k) for k in range(chips) for c in range(2)])

    chain.clear()
    x, dy = x[0], dy[0]
    g0 = gather(w_gate[0])
    a0, a0_turned = normed(x)
    u0 = gather(after(w_up[0], a0))
    (gate0,) = wide_call(gate_kernel, a0, g0, False, (), (F32,))
    d0 = gather(after(w_down[0], gate0))
    up0, act0 = wide_call(up_kernel, a0, u0, False, (gate0,), (F32, BF16))
    g1 = gather(after(w_gate[1], up0))
    h1, a1, a1_turned = down(x, act0, d0)
    u1 = gather(after(w_up[1], h1))
    (gate1,) = wide_call(gate_kernel, a1, g1, False, (), (F32,))
    d1 = gather(after(w_down[1], gate1))
    up1, act1 = wide_call(up_kernel, a1, u1, False, (gate1,), (F32, BF16))

    def back(act, a_turned, dh, w, gate, up):
        down_theirs = dw_tall(act, dh, other)
        dgate, dup = wide_call(back_kernel, dh, w, True, (gate, up), (BF16,) * 2)
        down_mine = dw_tall(act, dh, mine, swap(down_theirs))
        gate_theirs = dw_wide(a_turned, dgate, other)
        up_theirs = dw_wide(a_turned, dup, other)
        gate_mine = dw_wide(a_turned, dgate, mine, swap(gate_theirs))
        up_mine = dw_wide(a_turned, dup, mine, swap(up_theirs))
        return dgate, dup, *(scatter(t) for t in (down_mine, gate_mine, up_mine))

    dgate1, dup1, rs_d1, rs_g1, rs_u1 = back(act1, a1_turned, dy, d1, gate1, up1)
    dh1 = da_of(h1, dy, dgate1, dup1, g1, u1)
    dgate0, dup0, rs_d0, rs_g0, rs_u0 = back(act0, a0_turned, dh1, d0, gate0, up0)
    dx = da_of(x, dh1, dgate0, dup0, g0, u0)
    return (
        dx[None],
        jnp.stack((own_wide(rs_g0), own_wide(rs_g1))),
        jnp.stack((own_wide(rs_u0), own_wide(rs_u1))),
        jnp.stack((own_tall(rs_d0), own_tall(rs_d1))),
    )


def solution(mesh):
    cores = Mesh(mesh.devices.reshape(mesh.shape["rep"], -1, 2), ("rep", "chip", "core"))
    dp = ("chip", "core")
    seq = P(("rep", *dp), None, None)
    w = P(None, dp, None)
    out = P("rep", dp, None)
    return jax.shard_map(local, mesh=cores, in_specs=(seq, seq, w, w, w), out_specs=(seq, out, out, out), check_vma=False)
```
